16 devices in a mesh: pp: 2 (over z), ep: 8 (over y, x, core).
Axes of the slice: x: 2, y: 2, z: 2, core: 2. Of those that a mesh axis runs over, the one named last changes fastest.
Arguments:
- expert_out: bfloat16 [12, 128, 192, 2048], P('pp', 'ep')
- expert_ids: int32 [12, 8, 256, 8], P('pp', 'ep')
- slot_ids: int32 [12, 8, 256, 8], P('pp', 'ep')
- gate_vals: float32 [12, 8, 256, 8], P('pp', 'ep')
- residual: bfloat16 [12, 8, 256, 2048], P('pp', 'ep')
- norm_w: float32 [2, 2048], P('pp')
- w_query: bfloat16 [2, 2048, 32, 128], P('pp')
- w_key: bfloat16 [2, 2048, 32, 128], P('pp')
- w_value: bfloat16 [2, 2048, 32, 128], P('pp')
- w_out: bfloat16 [2, 32, 128, 2048], P('pp')
Outputs:
- output: bfloat16 [12, 8, 256, 2048], P('pp', 'ep')
All inputs are finite; a program needn't handle non-finite values.
Results may differ from the reference program's by a relative error of at most 0.0136648.
Values are sent between devices in bfloat16 or wider.
A program may use at most 1 GiB of HBM per device.

```python
import jax
import jax.numpy as jnp
from jax import lax

STAGES = 2
GROUP_SIZE = 8
NUM_MICRO = 6
SEQ_LEN = 256
SEQS_PER_DEV = 1
D_MODEL = 2048
NUM_EXPERTS = 128
TOP_K = 8
NUM_HEADS = 32
HEAD_DIM = 128
SRC_SLOTS = 24

TOKENS_DEV = SEQS_PER_DEV * SEQ_LEN
SEQS_ALL = GROUP_SIZE * SEQS_PER_DEV
CAPACITY = GROUP_SIZE * SRC_SLOTS
NUM_ROWS = STAGES * NUM_MICRO
QKV_WIDTH = NUM_HEADS * HEAD_DIM
NORM_EPS = 1e-6


def block_ranks(block_ids):
    perm_order = jnp.argsort(block_ids, stable=True)
    sorted_ids = block_ids[perm_order]
    group_start = jnp.searchsorted(sorted_ids, sorted_ids, side='left')
    rank_sorted = jnp.arange(block_ids.shape[0]) - group_start
    return jnp.zeros_like(block_ids).at[perm_order].set(rank_sorted)


def draw_routing(route_key):
    key_bias, key_hot, key_shift, key_noise, key_order = jax.random.split(route_key, 5)
    expert_bias = jnp.sum(jax.random.randint(key_bias, (NUM_ROWS, NUM_EXPERTS, 4), 0, 166, jnp.int32), axis=-1)
    hot_expert = jax.random.randint(key_hot, (NUM_ROWS,), 0, NUM_EXPERTS)
    cover_shift = jax.random.randint(key_shift, (NUM_ROWS,), 0, NUM_EXPERTS)
    local_pos = jnp.arange(TOKENS_DEV)
    expert_pos = jnp.arange(NUM_EXPERTS)
    tie_break = (NUM_EXPERTS - 1 - expert_pos).astype(jnp.int32)

    def one_block(flat_idx):
        row_idx = flat_idx // GROUP_SIZE
        blk_idx = flat_idx % GROUP_SIZE
        noise_draws = jnp.sum(jax.random.randint(jax.random.fold_in(key_noise, flat_idx), (TOKENS_DEV, NUM_EXPERTS, 3), 0, 164, jnp.int32), axis=-1)
        token_pos = blk_idx * TOKENS_DEV + local_pos
        is_cover = (token_pos[:, None] + cover_shift[row_idx]) % NUM_EXPERTS == expert_pos[None, :]
        is_hot = expert_pos[None, :] == hot_expert[row_idx]
        score_int = (expert_bias[row_idx][None, :] + noise_draws) * NUM_EXPERTS + tie_break[None, :] + (1 << 22) * is_cover.astype(jnp.int32) + (1 << 23) * is_hot.astype(jnp.int32)
        chosen = lax.top_k(score_int, TOP_K)[1]
        order_bits = jax.random.bits(jax.random.fold_in(key_order, flat_idx), (TOKENS_DEV, TOP_K), jnp.uint32) >> 8
        order_key = order_bits * TOP_K + jnp.arange(TOP_K, dtype=jnp.uint32)[None, :]
        perm_order = jnp.argsort(order_key, axis=1)
        chosen = jnp.take_along_axis(chosen, perm_order, axis=1)
        slot_rank = block_ranks(chosen.reshape(TOKENS_DEV * TOP_K)).reshape(TOKENS_DEV, TOP_K)
        slot_ids = jnp.where(slot_rank < SRC_SLOTS, blk_idx * SRC_SLOTS + slot_rank, -1)
        return chosen.astype(jnp.int32), slot_ids.astype(jnp.int32)

    expert_ids, slot_ids = lax.map(one_block, jnp.arange(NUM_ROWS * GROUP_SIZE))
    route_shape = (NUM_ROWS, SEQS_ALL, SEQ_LEN, TOP_K)
    return expert_ids.reshape(route_shape), slot_ids.reshape(route_shape)


def draw_bf16(draw_key, arr_shape, scale_fac):
    def one_slice(slice_key):
        return (scale_fac * jax.random.normal(slice_key, arr_shape[1:], jnp.float32)).astype(jnp.bfloat16)
    return lax.map(one_slice, jax.random.split(draw_key, arr_shape[0]))


def setup_inputs(seed: int = 0) -> dict:
    root_key = jax.random.key(seed)
    sub_keys = jax.random.split(root_key, 10)
    expert_ids, slot_ids = draw_routing(sub_keys[0])
    gate_vals = jax.nn.softmax(1.5 * jax.random.normal(sub_keys[1], (NUM_ROWS, SEQS_ALL, SEQ_LEN, TOP_K), jnp.float32), axis=-1)
    expert_scale = 1.5 * jnp.exp(0.5 * jax.random.normal(sub_keys[2], (NUM_ROWS * NUM_EXPERTS,), jnp.float32))

    def expert_slab(slab_args):
        slab_key, slab_scale = slab_args
        return (slab_scale * jax.random.normal(slab_key, (CAPACITY, D_MODEL), jnp.float32)).astype(jnp.bfloat16)

    expert_out = lax.map(expert_slab, (jax.random.split(sub_keys[3], NUM_ROWS * NUM_EXPERTS), expert_scale))
    expert_out = expert_out.reshape(NUM_ROWS, NUM_EXPERTS, CAPACITY, D_MODEL)
    residual = draw_bf16(sub_keys[4], (NUM_ROWS * SEQS_ALL, SEQ_LEN, D_MODEL), 1.0)
    residual = residual.reshape(NUM_ROWS, SEQS_ALL, SEQ_LEN, D_MODEL)
    norm_w = 1.0 + 0.4 * jax.random.normal(sub_keys[5], (STAGES, D_MODEL), jnp.float32)
    in_scale = D_MODEL ** -0.5
    out_scale = QKV_WIDTH ** -0.5
    w_query = draw_bf16(sub_keys[6], (STAGES, D_MODEL, NUM_HEADS, HEAD_DIM), 1.5 * in_scale)
    w_key = draw_bf16(sub_keys[7], (STAGES, D_MODEL, NUM_HEADS, HEAD_DIM), 1.5 * in_scale)
    w_value = draw_bf16(sub_keys[8], (STAGES, D_MODEL, NUM_HEADS, HEAD_DIM), in_scale)
    w_out = draw_bf16(sub_keys[9], (STAGES, NUM_HEADS, HEAD_DIM, D_MODEL), out_scale)
    return dict(expert_out=expert_out, expert_ids=expert_ids, slot_ids=slot_ids, gate_vals=gate_vals, residual=residual, norm_w=norm_w, w_query=w_query, w_key=w_key, w_value=w_value, w_out=w_out)


def reference(expert_out, expert_ids, slot_ids, gate_vals, residual, norm_w, w_query, w_key, w_value, w_out):
    causal = jnp.arange(SEQ_LEN)[:, None] >= jnp.arange(SEQ_LEN)[None, :]

    def one_stage(stage_idx):
        src_stage = (stage_idx + STAGES - 1) % STAGES
        stage_norm = norm_w[stage_idx]
        stage_wq = w_query[stage_idx].reshape(D_MODEL, QKV_WIDTH)
        stage_wk = w_key[stage_idx].reshape(D_MODEL, QKV_WIDTH)
        stage_wv = w_value[stage_idx].reshape(D_MODEL, QKV_WIDTH)
        stage_wo = w_out[stage_idx].reshape(QKV_WIDTH, D_MODEL)

        def project(x_in, weight_mat):
            head_out = jnp.dot(x_in, weight_mat, preferred_element_type=jnp.float32).astype(jnp.bfloat16)
            return head_out.reshape(SEQ_LEN, NUM_HEADS, HEAD_DIM).astype(jnp.float32)

        def one_sequence(flat_idx):
            src_row = src_stage * NUM_MICRO + flat_idx // SEQS_ALL
            seq_idx = flat_idx % SEQS_ALL
            ids_seq = expert_ids[src_row, seq_idx]
            slot_seq = slot_ids[src_row, seq_idx]
            is_kept = slot_seq >= 0
            picked = expert_out[src_row, ids_seq, jnp.where(is_kept, slot_seq, 0)].astype(jnp.float32)
            weight = jnp.where(is_kept, gate_vals[src_row, seq_idx], 0.0)
            mixed_sum = residual[src_row, seq_idx].astype(jnp.float32) + jnp.sum(weight[:, :, None] * picked, axis=1)
            y_wide = mixed_sum.astype(jnp.bfloat16).astype(jnp.float32)
            inv_rms = lax.rsqrt(jnp.mean(y_wide * y_wide, axis=-1, keepdims=True) + NORM_EPS)
            x_in = (y_wide * inv_rms * stage_norm).astype(jnp.bfloat16)
            q_heads = project(x_in, stage_wq)
            k_heads = project(x_in, stage_wk)
            v_heads = project(x_in, stage_wv)
            scores = jnp.einsum('qhe,khe->hqk', q_heads, k_heads) * HEAD_DIM ** -0.5
            attn_probs = jax.nn.softmax(jnp.where(causal, scores, -jnp.inf), axis=-1).astype(jnp.bfloat16)
            attn_out = jnp.einsum('hqk,khe->qhe', attn_probs.astype(jnp.float32), v_heads).astype(jnp.bfloat16)
            out_proj = jnp.dot(attn_out.reshape(SEQ_LEN, QKV_WIDTH), stage_wo, preferred_element_type=jnp.float32).astype(jnp.bfloat16)
            return (y_wide + out_proj.astype(jnp.float32)).astype(jnp.bfloat16)

        return lax.map(one_sequence, jnp.arange(NUM_MICRO * SEQS_ALL))

    stage_outs = lax.map(one_stage, jnp.arange(STAGES))
    return stage_outs.reshape(NUM_ROWS, SEQS_ALL, SEQ_LEN, D_MODEL)
```

```python
import functools

import jax
import jax.numpy as jnp
from jax import lax
from jax.experimental import pallas as pl
from jax.experimental.pallas import tpu as pltpu
from jax.sharding import PartitionSpec as P

NORM_EPS = 1e-6

CUTS = (0, 432, 752, 1088, 1392, 1712, 2016)
CHIP_STRIDE = 4096
TILE = 256
BF16, F32, I32 = jnp.bfloat16, jnp.float32, jnp.int32


def gated_sum(exp_table, expert_ids, slot_pos, gate_vals, residual):
    is_kept = slot_pos >= 0
    pick_rows = jax.vmap(lambda exp_rows, id_blk, pos_blk: exp_rows[id_blk, pos_blk])
    picked = pick_rows(exp_table, expert_ids, jnp.where(is_kept, slot_pos, 0))
    weight = jnp.where(is_kept, gate_vals, 0.0)
    mixed_sum = residual.astype(F32) + jnp.sum(weight[..., None] * picked.astype(F32), axis=3)
    return mixed_sum.astype(BF16)


def attention_block(combined, norm_w, w_query, w_key, w_value, w_out):
    y_wide = combined.astype(F32)
    inv_rms = lax.rsqrt(jnp.mean(y_wide * y_wide, axis=-1, keepdims=True) + NORM_EPS)
    x_in = (y_wide * inv_rms * norm_w).astype(BF16)
    q_heads = jnp.einsum('bld,dhe->blhe', x_in, w_query, preferred_element_type=F32).astype(BF16)
    k_heads = jnp.einsum('bld,dhe->blhe', x_in, w_key, preferred_element_type=F32).astype(BF16)
    v_heads = jnp.einsum('bld,dhe->blhe', x_in, w_value, preferred_element_type=F32).astype(BF16)
    head_dim = w_query.shape[2]
    seq_len = combined.shape[1]
    scores = jnp.einsum('bqhe,bkhe->bhqk', q_heads, k_heads, preferred_element_type=F32) * (head_dim ** -0.5)
    causal = jnp.arange(seq_len)[:, None] >= jnp.arange(seq_len)[None, :]
    attn_probs = jax.nn.softmax(jnp.where(causal, scores, -jnp.inf), axis=-1).astype(BF16)
    attn_out = jnp.einsum('bhqk,bkhe->bqhe', attn_probs, v_heads, preferred_element_type=F32).astype(BF16)
    out_proj = jnp.einsum('crif,ife->cre', attn_out, w_out, preferred_element_type=F32).astype(BF16)
    return (y_wide + out_proj.astype(F32)).astype(BF16)


def pack_body(num_rows, base, cap, _dv, *refs):
    per = 2 * num_rows
    blocks = (refs[:per], refs[per:2 * per])
    places = (refs[2 * per:2 * per + num_rows], refs[2 * per + num_rows:3 * per])
    outs = refs[3 * per:3 * per + 2]
    picks = refs[3 * per + 2]
    width = refs[0].shape[1] * refs[0].shape[2]

    @pl.when(pl.program_id(1) == 0)
    def _():
        for side in range(2):
            for row in range(num_rows):
                for core in range(2):
                    want = places[side][row][0, 0, :, core * width:(core + 1) * width]
                    have = lax.broadcasted_iota(I32, (cap, width), 0) + base
                    picks[side, 2 * row + core] = jnp.where(have == want, 1.0, 0.0).astype(BF16)

    for side in range(2):
        total = None
        for k in range(per):
            slots = blocks[side][k][...].reshape(width, TILE)
            part = jnp.dot(picks[side, k], slots, preferred_element_type=F32)
            total = part if total is None else total + part
        outs[side][0] = total.astype(BF16)


def pack_chunk(dv, expert_out, sib, places, rows, base, cap):
    num_exp, src_slots = expert_out.shape[1], expert_out.shape[2] // 8
    width = num_exp * src_slots
    half = expert_out.shape[3] // 2
    nt = half // TILE

    def dest(side, i, dv):
        return jnp.where(i == 0, dv[1 + side], dv[3])

    def own_map(side, row):
        return lambda i, n, dv: (row, 0, dest(side, i, dv), (1 - side) * nt + n)

    def sib_map(side):
        return lambda i, n, dv: (0, dest(side, i, dv) // 2, 0, (1 - side) * nt + n)

    in_specs, args = [], []
    for side in range(2):
        for row in rows:
            in_specs.append(pl.BlockSpec((1, num_exp, src_slots, TILE), own_map(side, row)))
            args.append(expert_out)
            in_specs.append(pl.BlockSpec((num_exp, 1, src_slots, TILE), sib_map(side)))
            args.append(sib[row])
    for side in range(2):
        for row in rows:
            in_specs.append(pl.BlockSpec((1, 1, 1, 2 * width), lambda i, n, dv, side=side, row=row: (jnp.where(i == 0, side, 2), row, 0, 0)))
            args.append(places)
    out = jax.ShapeDtypeStruct((2, cap, half), BF16)
    return pl.pallas_call(
        functools.partial(pack_body, len(rows), base, cap),
        out_shape=(out, out),
        grid_spec=pltpu.PrefetchScalarGridSpec(
            num_scalar_prefetch=1, grid=(2, nt), in_specs=in_specs,
            out_specs=[pl.BlockSpec((1, cap, TILE), lambda i, n, dv: (i, 0, n))] * 2,
            scratch_shapes=[pltpu.VMEM((2, 2 * len(rows), cap, width), BF16)]),
        compiler_params=pltpu.CompilerParams(dimension_semantics=("arbitrary", "arbitrary"), vmem_limit_bytes=60 << 20),
        cost_estimate=pl.CostEstimate(flops=2 * 4 * 2 * len(rows) * width * cap * half, bytes_accessed=4 * 2 * len(rows) * width * half * 2 + 4 * cap * half * 2, transcendentals=0),
        name="pack",
    )(dv, *args)


def fill_gates(lhs, at, meta, which, base, width):
    tokens = meta.shape[-1]
    place = meta[which, 0].T
    gate = meta[2, 0].T
    cols = lax.broadcasted_iota(I32, (tokens, width), 1).astype(F32)
    acc = jnp.zeros((tokens, width), F32)
    for i in range(place.shape[1]):
        acc = acc + jnp.where(place[:, i:i + 1] - base == cols, gate[:, i:i + 1], 0.0)
    for part in range(3):
        piece = acc.astype(BF16)
        lhs[part * tokens:(part + 1) * tokens, at:at + width] = piece
        acc = acc - piece.astype(F32)


def mixed(lhs, tokens, pieces):
    total = None
    for at, rows in pieces:
        part = jnp.dot(lhs[:, at:at + rows.shape[0]], rows, preferred_element_type=F32)
        total = part if total is None else total + part
    return total[:tokens] + total[tokens:2 * tokens] + total[2 * tokens:]


def layout(width, chunks):
    at, spots = 0, []
    for size in (width, width) + tuple(cap for _, cap in chunks):
        spots.append(at)
        at += -(-size // 128) * 128
    return spots, at


def mid_body(chunks, width, dv, meta_x, meta_y, own_a, sib_a, own_b, sib_b, *refs):
    nc = len(chunks)
    leaf_a, leaf_b = refs[:nc], refs[nc:2 * nc]
    out_a, out_b, lhs_a, lhs_b = refs[2 * nc:]
    tokens = meta_x.shape[-1]
    spots, _ = layout(width, chunks)

    @pl.when(pl.program_id(0) == 0)
    def _():
        for lhs, meta, chip in ((lhs_a, meta_x, dv[7]), (lhs_b, meta_y, dv[6])):
            fill_gates(lhs, spots[0], meta, 0, dv[4].astype(F32), width)
            fill_gates(lhs, spots[1], meta, 0, dv[5].astype(F32), width)
            for k, (base, cap) in enumerate(chunks):
                fill_gates(lhs, spots[2 + k], meta, 1, (chip + base).astype(F32), cap)

    for lhs, own, sib, leaf, out in ((lhs_a, own_a, sib_a, leaf_a, out_a), (lhs_b, own_b, sib_b, leaf_b, out_b)):
        pieces = [(spots[0], own[...].reshape(width, TILE)), (spots[1], sib[...].reshape(width, TILE))]
        pieces += [(spots[2 + k], leaf[k][0]) for k in range(nc)]
        out[...] = mixed(lhs, tokens, pieces)


def mid_sums(dv, row, meta_x, meta_y, expert_out, sib, leaf_x, leaf_y, chunk_ids):
    num_exp, src_slots = expert_out.shape[1], expert_out.shape[2] // 8
    width = num_exp * src_slots
    half = expert_out.shape[3] // 2
    nt = half // TILE
    tokens, choices = meta_x.shape[3], meta_x.shape[2]
    chunks = [(CUTS[c], CUTS[c + 1] - CUTS[c]) for c in chunk_ids]
    meta_spec = pl.BlockSpec((3, 1, choices, tokens), lambda n, dv: (0, row, 0, 0))
    in_specs = [meta_spec, meta_spec]
    args = [meta_x, meta_y]
    for side in range(2):
        in_specs.append(pl.BlockSpec((1, num_exp, src_slots, TILE), lambda n, dv, side=side: (row, 0, dv[1 + side], side * nt + n)))
        args.append(expert_out)
        in_specs.append(pl.BlockSpec((num_exp, 1, src_slots, TILE), lambda n, dv, side=side: (0, dv[1 + side] // 2, 0, side * nt + n)))
        args.append(sib[row])
    for leaf in (leaf_y, leaf_x):
        for c in chunk_ids:
            in_specs.append(pl.BlockSpec((1, CUTS[c + 1] - CUTS[c], TILE), lambda n, dv: (1, 0, n)))
            args.append(leaf[c])
    _, total = layout(width, chunks)
    out = jax.ShapeDtypeStruct((tokens, half), F32)
    return pl.pallas_call(
        functools.partial(mid_body, chunks, width),
        out_shape=(out, out),
        grid_spec=pltpu.PrefetchScalarGridSpec(
            num_scalar_prefetch=1, grid=(nt,), in_specs=in_specs,
            out_specs=[pl.BlockSpec((tokens, TILE), lambda n, dv: (0, n))] * 2,
            scratch_shapes=[pltpu.VMEM((3 * tokens, total), BF16)] * 2),
        compiler_params=pltpu.CompilerParams(dimension_semantics=("arbitrary",), vmem_limit_bytes=60 << 20),
        cost_estimate=pl.CostEstimate(flops=2 * 2 * 3 * tokens * total * half, bytes_accessed=2 * total * half * 2 + 2 * tokens * half * 4, transcendentals=0),
        name="mid",
    )(dv, *args)


def fin_body(chunks, width, nt, dv, meta, own, sib, *refs):
    nc = len(chunks)
    leaf_a, leaf_b = refs[:nc], refs[nc:2 * nc]
    part_a, part_b, resid, out, lhs = refs[2 * nc:]
    tokens = meta.shape[-1]
    spots, total = layout(width, list(chunks) * 2)
    step = pl.program_id(0)

    @pl.when(step == 0)
    def _():
        fill_gates(lhs, spots[0], meta, 0, dv[4].astype(F32), width)
        fill_gates(lhs, spots[1], meta, 0, dv[5].astype(F32), width)
        for side, chip in ((0, dv[7]), (1, dv[6])):
            for k, (base, cap) in enumerate(chunks):
                fill_gates(lhs, spots[2 + side * nc + k], meta, 1, (chip + base).astype(F32), cap)

    for side, leaf, part in ((0, leaf_a, part_a), (1, leaf_b, part_b)):
        @pl.when(step // nt == side)
        def _(side=side, leaf=leaf, part=part):
            pieces = [(spots[0], own[...].reshape(width, TILE)), (spots[1], sib[...].reshape(width, TILE))]
            pieces += [(spots[2 + side * nc + k], leaf[k][0]) for k in range(nc)]
            out[...] = (resid[0, 0].astype(F32) + (mixed(lhs, tokens, pieces) + part[...])).astype(BF16)


def fin_sums(dv, row, meta, expert_out, sib, leaf_x, leaf_y, chunk_ids, part_a, part_b, residual):
    num_exp, src_slots = expert_out.shape[1], expert_out.shape[2] // 8
    width = num_exp * src_slots
    d_model = expert_out.shape[3]
    nt = d_model // 2 // TILE
    tokens, choices = meta.shape[3], meta.shape[2]
    chunks = [(CUTS[c], CUTS[c + 1] - CUTS[c]) for c in chunk_ids]
    lo = lambda n: jnp.minimum(n, nt - 1)
    hi = lambda n: jnp.maximum(n - nt, 0)
    in_specs = [
        pl.BlockSpec((3, 1, choices, tokens), lambda n, dv: (0, row, 0, 0)),
        pl.BlockSpec((1, num_exp, src_slots, TILE), lambda n, dv: (row, 0, dv[0], n)),
        pl.BlockSpec((num_exp, 1, src_slots, TILE), lambda n, dv: (0, dv[0] // 2, 0, n)),
    ]
    args = [meta, expert_out, sib[row]]
    for leaf, pick in ((leaf_y, lo), (leaf_x, hi)):
        for c in chunk_ids:
            in_specs.append(pl.BlockSpec((1, CUTS[c + 1] - CUTS[c], TILE), lambda n, dv, pick=pick: (0, 0, pick(n))))
            args.append(leaf[c])
    in_specs += [
        pl.BlockSpec((tokens, TILE), lambda n, dv: (0, lo(n))),
        pl.BlockSpec((tokens, TILE), lambda n, dv: (0, hi(n))),
        pl.BlockSpec((1, 1, tokens, TILE), lambda n, dv: (row, 0, 0, n)),
    ]
    args += [part_a, part_b, residual]
    _, total = layout(width, list(chunks) * 2)
    return pl.pallas_call(
        functools.partial(fin_body, chunks, width, nt),
        out_shape=jax.ShapeDtypeStruct((tokens, d_model), BF16),
        grid_spec=pltpu.PrefetchScalarGridSpec(
            num_scalar_prefetch=1, grid=(2 * nt,), in_specs=in_specs,
            out_specs=pl.BlockSpec((tokens, TILE), lambda n, dv: (0, n)),
            scratch_shapes=[pltpu.VMEM((3 * tokens, total), BF16)]),
        compiler_params=pltpu.CompilerParams(dimension_semantics=("arbitrary",), vmem_limit_bytes=60 << 20),
        cost_estimate=pl.CostEstimate(flops=2 * 3 * tokens * total * d_model, bytes_accessed=total * d_model * 2 + 3 * tokens * d_model * 4, transcendentals=0),
        name="fin",
    )(dv, *args)


def routing(expert_ids, slot_ids, gate_vals, me, pp):
    rows, tokens, choices = expert_ids.shape
    num_chips, per_chip, per_dev, src_slots = 4, 32, 16, 24
    num_exp = num_chips * per_chip
    kept = slot_ids >= 0
    rank = slot_ids - me * src_slots
    onehot = expert_ids[..., None] == jnp.arange(num_exp, dtype=I32)
    count = jnp.sum((onehot & kept[..., None]).astype(I32), axis=(1, 2))
    by_chip = count.reshape(rows, num_chips, per_chip)
    before = jnp.arange(per_chip)[:, None] < jnp.arange(per_chip)[None, :]
    inner = jnp.sum(jnp.where(before, by_chip[..., None], 0), axis=2)
    totals = jnp.sum(by_chip, axis=2)
    starts, end = [], jnp.zeros((num_chips,), I32)
    spill = jnp.zeros((num_chips,), I32)
    foreign = jnp.arange(num_chips) != me // 2
    for r in range(rows):
        start = jnp.maximum(end, CUTS[max(r - 1, 0)])
        end = start + totals[r]
        spill = jnp.maximum(spill, (end > CUTS[r + 1]).astype(I32))
        starts.append(start)
    spill = jnp.max(jnp.where(foreign, spill, 0))
    base = (jnp.stack(starts)[:, :, None] + inner).reshape(rows, num_exp)
    table = jnp.concatenate([base, count, jnp.full((1, num_exp), spill, I32)], axis=0)
    everyone = lax.all_gather(table, ('pp', 'ep'))
    overflow = jnp.max(everyone[:, 2 * rows, 0]) > 0
    chip = expert_ids // per_chip
    home = jnp.sum(jnp.where(onehot, base[:, None, None, :], 0), axis=3)
    stream = jnp.where(kept, chip * CHIP_STRIDE + home + rank, -1)
    dense = jnp.where(kept, expert_ids * src_slots + rank, -1)
    meta = jnp.stack([dense.astype(F32), stream.astype(F32), gate_vals])
    meta = meta.transpose(0, 1, 3, 2)
    stage = lax.dynamic_slice_in_dim(everyone, pp * 8, 8, 0)
    places = []
    col = jnp.arange(per_dev * src_slots, dtype=I32)
    spread = (col[None, :] // src_slots) == jnp.arange(per_dev, dtype=I32)[:, None]
    slot = col % src_slots
    for m in (2, 4, 6):
        one = lax.dynamic_index_in_dim(stage, me ^ m, 0, keepdims=False)
        parts = []
        for dev in (me, me ^ 1):
            mine = lax.dynamic_slice_in_dim(one, dev * per_dev, per_dev, 1)
            wide = jnp.sum(jnp.where(spread, mine[:, :, None], 0), axis=1)
            parts.append(jnp.where(slot < wide[rows:2 * rows], wide[:rows] + slot, -1))
        places.append(jnp.concatenate(parts, axis=1))
    return meta, jnp.stack(places)[:, :, None, :], overflow


def solution(mesh):
    stages = mesh.shape['pp']
    group_size = mesh.shape['ep']
    send_next = [(src_row, (src_row + 1) % stages) for src_row in range(stages)]
    tok_spec = P('pp', 'ep', None, None)
    wt_spec = P('pp', None, None, None)

    def across(x, m):
        return lax.ppermute(x, 'ep', [(i, i ^ m) for i in range(group_size)])

    def dense_path(expert_out, expert_ids, slot_ids, gate_vals, residual, norm_w, w_query, w_key, w_value, w_out):
        num_micro, seqs_dev, seq_len, d_model = residual.shape
        src_slots = expert_out.shape[2] // group_size
        returned = lax.all_to_all(expert_out, 'ep', 2, 1, tiled=True)
        block_base = lax.axis_index('ep') * src_slots
        slot_pos = jnp.where(slot_ids >= 0, slot_ids - block_base, -1)
        combined = gated_sum(returned, expert_ids, slot_pos, gate_vals, residual)
        arrived = lax.ppermute(combined, 'pp', send_next)
        flat_in = arrived.reshape(num_micro * seqs_dev, seq_len, d_model)
        result = attention_block(flat_in, norm_w[0], w_query[0], w_key[0], w_value[0], w_out[0])
        return result.reshape(num_micro, seqs_dev, seq_len, d_model)

    def device_step(expert_out, expert_ids, slot_ids, gate_vals, residual, norm_w, w_query, w_key, w_value, w_out):
        num_micro = residual.shape[0]
        me, pp = lax.axis_index('ep'), lax.axis_index('pp')
        num_exp, cap = expert_out.shape[1:3]
        d_model = expert_out.shape[3]
        src_slots = cap // group_size
        by_core = expert_out.reshape(num_micro, num_exp, group_size // 2, 2, src_slots, d_model)

        def sibling(r):
            return across(lax.dynamic_index_in_dim(by_core[r], 1 - me % 2, 2, keepdims=False), 1)

        meta, places, overflow = routing(expert_ids[:, 0], slot_ids[:, 0], gate_vals[:, 0], me, pp)
        width = num_exp * src_slots
        dv = jnp.stack([me, me ^ 2, me ^ 4, me ^ 6, me * width, (me ^ 1) * width, (me ^ 2) // 2 * CHIP_STRIDE, (me ^ 4) // 2 * CHIP_STRIDE])

        def packed_path(meta, places, dv, expert_out, expert_ids, slot_ids, gate_vals, residual, norm_w, w_query, w_key, w_value, w_out):
            meta_x, meta_y = across(meta, 2), across(meta, 4)
            sib = [sibling(r) for r in range(num_micro)]
            leaf_x, leaf_y = [], []
            for c in range(num_micro):
                rows = [r for r in (c, c + 1) if r < num_micro]
                to_x, to_y = pack_chunk(dv, expert_out, sib, places, rows, CUTS[c], CUTS[c + 1] - CUTS[c])
                leaf_x.append(across(to_x, 2))
                leaf_y.append(across(to_y, 4))
            outs = []
            for r in range(num_micro):
                chunk_ids = [c for c in (r - 1, r) if c >= 0]
                part_a, part_b = mid_sums(dv, r, meta_x, meta_y, expert_out, sib, leaf_x, leaf_y, chunk_ids)
                part_a, part_b = across(part_a, 2), across(part_b, 4)
                y = fin_sums(dv, r, meta, expert_out, sib, leaf_x, leaf_y, chunk_ids, part_a, part_b, residual)
                arrived = lax.ppermute(y, 'pp', send_next)
                outs.append(attention_block(arrived[None], norm_w[0], w_query[0], w_key[0], w_value[0], w_out[0]))
            return jnp.stack(outs)

        args = (expert_out, expert_ids, slot_ids, gate_vals, residual, norm_w, w_query, w_key, w_value, w_out)
        return lax.cond(overflow, lambda meta, places, dv, *a: dense_path(*a), packed_path, meta, places, dv, *args)

    return jax.shard_map(device_step, mesh=mesh, in_specs=(tok_spec, tok_spec, tok_spec, tok_spec, tok_spec, P('pp', None), wt_spec, wt_spec, wt_spec, wt_spec), out_specs=tok_spec, check_vma=False)
```

```python
import functools

import jax
import jax.numpy as jnp
from jax import lax
from jax.experimental import pallas as pl
from jax.experimental.pallas import tpu as pltpu
from jax.sharding import PartitionSpec as P

NORM_EPS = 1e-6

CUTS = (0, 512, 768, 1152, 1408, 1792, 2048)
CHIP_STRIDE = 4096
VMEM_LIMIT = 63 << 20
TILE = 512


def cost(macs, moved):
    return pl.CostEstimate(flops=2 * macs, bytes_accessed=2 * moved, transcendentals=0)


TOKEN = pl.BlockSpec(memory_space=pl.ANY)
BF16, F32, I32 = jnp.bfloat16, jnp.float32, jnp.int32


def gated_sum(exp_table, expert_ids, slot_pos, gate_vals, residual):
    is_kept = slot_pos >= 0
    pick_rows = jax.vmap(lambda exp_rows, id_blk, pos_blk: exp_rows[id_blk, pos_blk])
    picked = pick_rows(exp_table, expert_ids, jnp.where(is_kept, slot_pos, 0))
    weight = jnp.where(is_kept, gate_vals, 0.0)
    mixed_sum = residual.astype(F32) + jnp.sum(weight[..., None] * picked.astype(F32), axis=3)
    return mixed_sum.astype(BF16)


def attention_block(combined, norm_w, w_query, w_key, w_value, w_out):
    y_wide = combined.astype(F32)
    inv_rms = lax.rsqrt(jnp.mean(y_wide * y_wide, axis=-1, keepdims=True) + NORM_EPS)
    x_in = (y_wide * inv_rms * norm_w).astype(BF16)
    q_heads = jnp.einsum('bld,dhe->blhe', x_in, w_query, preferred_element_type=F32).astype(BF16)
    k_heads = jnp.einsum('bld,dhe->blhe', x_in, w_key, preferred_element_type=F32).astype(BF16)
    v_heads = jnp.einsum('bld,dhe->blhe', x_in, w_value, preferred_element_type=F32).astype(BF16)
    head_dim = w_query.shape[2]
    seq_len = combined.shape[1]
    scores = jnp.einsum('bqhe,bkhe->bhqk', q_heads, k_heads, preferred_element_type=F32) * (head_dim ** -0.5)
    causal = jnp.arange(seq_len)[:, None] >= jnp.arange(seq_len)[None, :]
    attn_probs = jax.nn.softmax(jnp.where(causal, scores, -jnp.inf), axis=-1).astype(BF16)
    attn_out = jnp.einsum('bhqk,bkhe->bqhe', attn_probs, v_heads, preferred_element_type=F32).astype(BF16)
    out_proj = jnp.einsum('crif,ife->cre', attn_out, w_out, preferred_element_type=F32).astype(BF16)
    return (y_wide + out_proj.astype(F32)).astype(BF16)


def route_body(me, idx, slot, table, choice_sum):
    rows, tokens, choices = idx.shape
    lanes = table.shape[1]
    choice_sum[:] = jnp.zeros_like(choice_sum)
    lane = lax.broadcasted_iota(I32, (tokens, lanes), 1)
    for r in range(rows):
        kept = jnp.where(slot[r] >= 0, idx[r], -1)
        hits = jnp.zeros((tokens, lanes), F32)
        for i in range(choices):
            hits = jnp.where(kept[:, i:i + 1] == lane, 1.0, hits)
        choice_sum[r:r + 1, :] = jnp.sum(hits, axis=0, keepdims=True)
    count = choice_sum[:]
    src = lax.broadcasted_iota(I32, (lanes, lanes), 0)
    dst = lax.broadcasted_iota(I32, (lanes, lanes), 1)
    same = src // 32 == dst // 32
    small = count.astype(BF16)
    inner = jnp.dot(small, jnp.where(same & (src < dst), 1.0, 0.0).astype(BF16), preferred_element_type=F32)
    total = jnp.dot(small, jnp.where(same, 1.0, 0.0).astype(BF16), preferred_element_type=F32)
    end = jnp.zeros((1, lanes), F32)
    spill = jnp.zeros((1, lanes), F32)
    base = []
    for r in range(rows):
        start = jnp.maximum(end, float(CUTS[max(r - 1, 0)]))
        end = start + total[r:r + 1]
        spill = jnp.where(end > float(CUTS[r + 1]), 1.0, spill)
        base.append(start + inner[r:r + 1])
    foreign = lax.broadcasted_iota(I32, (1, lanes), 1) // 32 != me[0] // 2
    spill = jnp.where(foreign, spill, 0.0)
    pad = jnp.zeros((8 - rows, lanes), F32)
    table[:] = jnp.concatenate(base + [pad, count[:rows], spill, pad[1:]], axis=0).astype(I32)


def route(me, idx, slot):
    whole = pl.BlockSpec(memory_space=pltpu.VMEM)
    return pl.pallas_call(
        route_body,
        out_shape=jax.ShapeDtypeStruct((16, 128), I32),
        in_specs=[pl.BlockSpec(memory_space=pltpu.SMEM), whole, whole], out_specs=whole,
        scratch_shapes=[pltpu.VMEM((8, 128), F32)],
        compiler_params=pltpu.CompilerParams(vmem_limit_bytes=VMEM_LIMIT),
        name="route",
    )(me[None], idx, slot)


def meta_body(me, _tok, idx, slot, gate, table, out):
    rows, tokens, choices = idx.shape
    lanes = table.shape[1]
    lane = lax.broadcasted_iota(I32, (tokens, lanes), 1)
    col = lax.broadcasted_iota(I32, (tokens, choices), 1)
    base = table[:].astype(F32)
    for r in range(rows):
        home = jnp.zeros((tokens, choices), F32)
        for i in range(choices):
            here = jnp.sum(jnp.where(idx[r][:, i:i + 1] == lane, base[r:r + 1], 0.0), axis=1, keepdims=True)
            home = jnp.where(col == i, here, home)
        kept = slot[r] >= 0
        rank = slot[r] - me[0] * 24
        out[0, r] = jnp.where(kept, idx[r] * 24 + rank, -1).astype(F32).T
        out[1, r] = jnp.where(kept, (idx[r] // 32 * CHIP_STRIDE + rank).astype(F32) + home, -1.0).T
        out[2, r] = gate[r].T


def token_meta(me, tok, idx, slot, gate, table):
    rows, tokens, choices = idx.shape
    whole = pl.BlockSpec(memory_space=pltpu.VMEM)
    return pl.pallas_call(
        meta_body,
        out_shape=jax.ShapeDtypeStruct((3, rows, choices, tokens), F32),
        in_specs=[pl.BlockSpec(memory_space=pltpu.SMEM), TOKEN, whole, whole, whole, whole], out_specs=whole,
        compiler_params=pltpu.CompilerParams(vmem_limit_bytes=VMEM_LIMIT),
        name="meta",
    )(me[None], tok, idx, slot, gate, table)


def places_body(where, everyone, out):
    me, first = where[0], where[1]
    width = out.shape[1] // 2
    lanes = everyone.shape[2]
    col = lax.broadcasted_iota(I32, (lanes, 2 * width), 1)
    exp = lax.broadcasted_iota(I32, (lanes, 2 * width), 0)
    own = me * 16 + col // 24
    sib = (me ^ 1) * 16 + (col - width) // 24
    spread = jnp.where(exp == jnp.where(col < width, own, sib), 1.0, 0.0).astype(BF16)
    slot = lax.broadcasted_iota(I32, (8, 2 * width), 1) % 24
    for k, m in enumerate((2, 4, 6)):
        one = everyone[first + (me ^ m)]
        high = one // 128
        wide = jnp.dot(high.astype(F32).astype(BF16), spread, preferred_element_type=F32) * 128.0
        wide = wide + jnp.dot((one - high * 128).astype(F32).astype(BF16), spread, preferred_element_type=F32)
        wide = wide.astype(I32)
        out[8 * k:8 * k + 8, :] = jnp.where(slot < wide[8:], wide[:8] + slot, -1)


def stream_places(me, pp, everyone, width):
    whole = pl.BlockSpec(memory_space=pltpu.VMEM)
    return pl.pallas_call(
        places_body,
        out_shape=jax.ShapeDtypeStruct((24, 2 * width), I32),
        in_specs=[pl.BlockSpec(memory_space=pltpu.SMEM), whole], out_specs=whole,
        compiler_params=pltpu.CompilerParams(vmem_limit_bytes=VMEM_LIMIT),
        name="places",
    )(jnp.stack([me, pp * 8]), everyone)


def copy_body(_dv, _tok, src, dst):
    dst[:] = src[:].reshape(dst.shape)


def sibling_slots(dv, tok, row, expert_out):
    num_exp, src_slots, d_model = expert_out.shape[1], expert_out.shape[2] // 8, expert_out.shape[3]
    out = jax.ShapeDtypeStruct((1, num_exp, 4, src_slots, d_model), BF16)
    return pl.pallas_call(
        copy_body,
        out_shape=out,
        grid_spec=pltpu.PrefetchScalarGridSpec(
            num_scalar_prefetch=1, grid=(4,),
            in_specs=[TOKEN, pl.BlockSpec((1, num_exp, src_slots, d_model), lambda q, dv: (row, 0, 2 * q + 1 - dv[0] % 2, 0))],
            out_specs=pl.BlockSpec((1, num_exp, 1, src_slots, d_model), lambda q, dv: (0, 0, q, 0, 0))),
        compiler_params=pltpu.CompilerParams(vmem_limit_bytes=VMEM_LIMIT),
        cost_estimate=cost(0, 2 * out.size),
        name="slots",
    )(dv, tok, expert_out)


def flat_body(_tok, *refs):
    num = len(refs) // 2
    for src, dst in zip(refs[:num], refs[num:]):
        dst[:] = src[0].reshape(dst.shape)


def flat_weights(tok, weights):
    d_model, heads, head_dim = weights[0].shape[1:]
    block = 128
    out = jax.ShapeDtypeStruct((d_model, heads * head_dim), BF16)
    return pl.pallas_call(
        flat_body,
        out_shape=[out] * len(weights),
        grid=(d_model // block,),
        in_specs=[TOKEN] + [pl.BlockSpec((1, block, heads, head_dim), lambda k: (0, k, 0, 0))] * len(weights),
        out_specs=[pl.BlockSpec((block, heads * head_dim), lambda k: (k, 0))] * len(weights),
        compiler_params=pltpu.CompilerParams(vmem_limit_bytes=VMEM_LIMIT),
        cost_estimate=cost(0, 2 * len(weights) * out.size),
        name="flat",
    )(tok, *weights)


def pack_body(rows, base, cap, _dv, _tok, *refs):
    per = 2 * len(rows)
    blocks = (refs[:per], refs[per:2 * per])
    places = refs[2 * per:2 * per + 2]
    outs = refs[2 * per + 2:2 * per + 4]
    picks = refs[2 * per + 4]
    width = refs[0].shape[1] * refs[0].shape[2]

    @pl.when(pl.program_id(1) == 0)
    def _():
        for side in range(2):
            for k, row in enumerate(rows):
                want = places[side][row:row + 1, :]
                have = lax.broadcasted_iota(I32, (cap, 2 * width), 0) + base
                picks[side, :, 2 * k * width:2 * (k + 1) * width] = jnp.where(have == want, 1.0, 0.0).astype(BF16)

    for side in range(2):
        slots = jnp.concatenate([block[:].reshape(width, TILE) for block in blocks[side]], axis=0)
        outs[side][0] = jnp.dot(picks[side], slots, preferred_element_type=F32).astype(BF16)


def pack_chunk(dv, tok, expert_out, sib, places, rows, base, cap):
    num_exp, src_slots = expert_out.shape[1], expert_out.shape[2] // 8
    width = num_exp * src_slots
    half = expert_out.shape[3] // 2
    nt = half // TILE

    def dest(side, i, dv):
        return jnp.where(i == 0, dv[1 + side], dv[3])

    in_specs, args = [TOKEN], [tok]
    for side in range(2):
        for row in rows:
            in_specs.append(pl.BlockSpec((1, num_exp, src_slots, TILE), lambda i, n, dv, side=side, row=row: (row, 0, dest(side, i, dv), (1 - side) * nt + n)))
            args.append(expert_out)
            in_specs.append(pl.BlockSpec((1, num_exp, 1, src_slots, TILE), lambda i, n, dv, side=side: (0, 0, dest(side, i, dv) // 2, 0, (1 - side) * nt + n)))
            args.append(sib[row])
    for side in range(2):
        in_specs.append(pl.BlockSpec((8, 2 * width), lambda i, n, dv, side=side: (jnp.where(i == 0, side, 2), 0)))
        args.append(places)
    out = jax.ShapeDtypeStruct((2, cap, half), BF16)
    return pl.pallas_call(
        functools.partial(pack_body, rows, base, cap),
        out_shape=(out, out),
        grid_spec=pltpu.PrefetchScalarGridSpec(
            num_scalar_prefetch=1, grid=(2, nt), in_specs=in_specs,
            out_specs=[pl.BlockSpec((1, cap, TILE), lambda i, n, dv: (i, 0, n))] * 2,
            scratch_shapes=[pltpu.VMEM((2, cap, 2 * len(rows) * width), BF16)]),
        compiler_params=pltpu.CompilerParams(vmem_limit_bytes=VMEM_LIMIT),
        cost_estimate=cost(8 * len(rows) * width * cap * half, 8 * len(rows) * width * half),
        name="pack",
    )(dv, *args)


def fill_gates(lhs, wide, meta, spans):
    tokens, choices = meta.shape[-1], meta.shape[-2]
    for which in range(3):
        value = meta[which, 0].T
        for i in range(choices):
            wide[which * choices + i] = jnp.broadcast_to(value[:, i:i + 1], (tokens, 128))
    step = 16
    lane = lax.broadcasted_iota(I32, (step, 128), 1).astype(F32)

    @pl.loop(0, tokens // step)
    def _(g):
        at_token = pl.multiple_of(g * step, step)
        gates = [wide[2 * choices + i, pl.ds(at_token, step), :] for i in range(choices)]
        for which in range(2):
            place = [wide[which * choices + i, pl.ds(at_token, step), :] for i in range(choices)]
            for at, kind, base, width in spans:
                if kind != which:
                    continue
                for tile in range(0, width, 128):
                    cols = lane + (base + tile).astype(F32)
                    acc = jnp.zeros((step, 128), F32)
                    for i in range(choices):
                        acc = jnp.where(place[i] == cols, gates[i], acc)
                    for part in range(3):
                        piece = acc.astype(BF16)
                        lhs[pl.ds(part * tokens + at_token, step), at + tile:at + tile + 128] = piece
                        acc = acc - piece.astype(F32)


def fold(total):
    tokens = total.shape[0] // 3
    return total[:tokens] + total[tokens:2 * tokens] + total[2 * tokens:]


def mid_body(chunks, width, dv, _tok, meta_x, meta_y, own_a, sib_a, own_b, sib_b, *refs):
    nc = len(chunks)
    leaf_a, leaf_b = refs[:nc], refs[nc:2 * nc]
    out_a, out_b, lhs_a, lhs_b, wide = refs[2 * nc:]

    @pl.when(pl.program_id(0) == 0)
    def _():
        for lhs, meta, chip in ((lhs_a, meta_x, dv[7]), (lhs_b, meta_y, dv[6])):
            spans, at = [(0, 0, dv[4], width), (width, 0, dv[5], width)], 2 * width
            for base, cap in chunks:
                spans.append((at, 1, chip + base, cap))
                at += cap
            fill_gates(lhs, wide, meta, spans)

    for lhs, own, sib, leaf, out in ((lhs_a, own_a, sib_a, leaf_a, out_a), (lhs_b, own_b, sib_b, leaf_b, out_b)):
        rows = jnp.concatenate([own[:].reshape(width, TILE), sib[:].reshape(width, TILE)] + [one[0] for one in leaf], axis=0)
        out[:] = fold(jnp.dot(lhs[:], rows, preferred_element_type=F32))


def mid_sums(dv, tok, row, meta_x, meta_y, expert_out, sib, leaf_x, leaf_y, chunk_ids):
    num_exp, src_slots = expert_out.shape[1], expert_out.shape[2] // 8
    width = num_exp * src_slots
    half = expert_out.shape[3] // 2
    nt = half // TILE
    tokens, choices = meta_x.shape[3], meta_x.shape[2]
    chunks = [(CUTS[c], CUTS[c + 1] - CUTS[c]) for c in chunk_ids]
    meta_spec = pl.BlockSpec((3, 1, choices, tokens), lambda n, dv: (0, row, 0, 0))
    in_specs = [TOKEN, meta_spec, meta_spec]
    args = [tok, meta_x, meta_y]
    for side in range(2):
        in_specs.append(pl.BlockSpec((1, num_exp, src_slots, TILE), lambda n, dv, side=side: (row, 0, dv[1 + side], side * nt + n)))
        args.append(expert_out)
        in_specs.append(pl.BlockSpec((1, num_exp, 1, src_slots, TILE), lambda n, dv, side=side: (0, 0, dv[1 + side] // 2, 0, side * nt + n)))
        args.append(sib[row])
    for leaf in (leaf_y, leaf_x):
        for c in chunk_ids:
            in_specs.append(pl.BlockSpec((1, CUTS[c + 1] - CUTS[c], TILE), lambda n, dv: (1, 0, n)))
            args.append(leaf[c])
    total = 2 * width + sum(cap for _, cap in chunks)
    out = jax.ShapeDtypeStruct((tokens, half), F32)
    return pl.pallas_call(
        functools.partial(mid_body, chunks, width),
        out_shape=(out, out),
        grid_spec=pltpu.PrefetchScalarGridSpec(
            num_scalar_prefetch=1, grid=(nt,), in_specs=in_specs,
            out_specs=[pl.BlockSpec((tokens, TILE), lambda n, dv: (0, n))] * 2,
            scratch_shapes=[pltpu.VMEM((3 * tokens, total), BF16)] * 2 + [pltpu.VMEM((3 * choices, tokens, 128), F32)]),
        compiler_params=pltpu.CompilerParams(vmem_limit_bytes=VMEM_LIMIT),
        cost_estimate=cost(6 * tokens * total * half, 2 * total * half),
        name="mid",
    )(dv, *args)


def fin_body(chunks, width, nt, dv, _tok, meta, own, sib, *refs):
    nc = len(chunks)
    leaf_a, leaf_b = refs[:nc], refs[nc:2 * nc]
    part_a, part_b, resid, out, lhs, wide = refs[2 * nc:]
    step = pl.program_id(0)
    extra = sum(cap for _, cap in chunks)

    @pl.when(step == 0)
    def _():
        spans, at = [(0, 0, dv[4], width), (width, 0, dv[5], width)], 2 * width
        for chip in (dv[7], dv[6]):
            for base, cap in chunks:
                spans.append((at, 1, chip + base, cap))
                at += cap
        fill_gates(lhs, wide, meta, spans)

    for side, leaf, part in ((0, leaf_a, part_a), (1, leaf_b, part_b)):
        @pl.when(step // nt == side)
        def _(side=side, leaf=leaf, part=part):
            near = jnp.concatenate([own[:].reshape(width, TILE), sib[:].reshape(width, TILE)], axis=0)
            far = jnp.concatenate([one[0] for one in leaf], axis=0)
            at = 2 * width + side * extra
            total = jnp.dot(lhs[:, :2 * width], near, preferred_element_type=F32) + jnp.dot(lhs[:, at:at + extra], far, preferred_element_type=F32)
            out[:] = (resid[0, 0].astype(F32) + (fold(total) + part[:])).astype(BF16)


def fin_sums(dv, tok, row, meta, expert_out, sib, leaf_x, leaf_y, chunk_ids, part_a, part_b, residual):
    num_exp, src_slots = expert_out.shape[1], expert_out.shape[2] // 8
    width = num_exp * src_slots
    d_model = expert_out.shape[3]
    nt = d_model // 2 // TILE
    tokens, choices = meta.shape[3], meta.shape[2]
    chunks = [(CUTS[c], CUTS[c + 1] - CUTS[c]) for c in chunk_ids]
    lo = lambda n: jnp.minimum(n, nt - 1)
    hi = lambda n: jnp.maximum(n - nt, 0)
    in_specs = [
        TOKEN,
        pl.BlockSpec((3, 1, choices, tokens), lambda n, dv: (0, row, 0, 0)),
        pl.BlockSpec((1, num_exp, src_slots, TILE), lambda n, dv: (row, 0, dv[0], n)),
        pl.BlockSpec((1, num_exp, 1, src_slots, TILE), lambda n, dv: (0, 0, dv[0] // 2, 0, n)),
    ]
    args = [tok, meta, expert_out, sib[row]]
    for leaf, pick in ((leaf_y, lo), (leaf_x, hi)):
        for c in chunk_ids:
            in_specs.append(pl.BlockSpec((1, CUTS[c + 1] - CUTS[c], TILE), lambda n, dv, pick=pick: (0, 0, pick(n))))
            args.append(leaf[c])
    in_specs += [
        pl.BlockSpec((tokens, TILE), lambda n, dv: (0, lo(n))),
        pl.BlockSpec((tokens, TILE), lambda n, dv: (0, hi(n))),
        pl.BlockSpec((1, 1, tokens, TILE), lambda n, dv: (row, 0, 0, n)),
    ]
    args += [part_a, part_b, residual]
    extra = sum(cap for _, cap in chunks)
    total = 2 * width + 2 * extra
    return pl.pallas_call(
        functools.partial(fin_body, chunks, width, nt),
        out_shape=jax.ShapeDtypeStruct((tokens, d_model), BF16),
        grid_spec=pltpu.PrefetchScalarGridSpec(
            num_scalar_prefetch=1, grid=(2 * nt,), in_specs=in_specs,
            out_specs=pl.BlockSpec((tokens, TILE), lambda n, dv: (0, n)),
            scratch_shapes=[pltpu.VMEM((3 * tokens, total), BF16), pltpu.VMEM((3 * choices, tokens, 128), F32)]),
        compiler_params=pltpu.CompilerParams(vmem_limit_bytes=VMEM_LIMIT),
        cost_estimate=cost(3 * tokens * total * d_model, total * d_model),
        name="fin",
    )(dv, *args)


def attn_body(num, _tok, *refs):
    ys, (norm_ref, wq, wk, wv, wo) = refs[:num], refs[num:num + 5]
    out, x_in, acc = refs[-3:]
    step, last = pl.program_id(0), pl.num_programs(0) - 1
    head_dim = 128
    tokens = ys[0].shape[0]

    @pl.when(step == 0)
    def _():
        for j in range(num):
            y_wide = ys[j][:].astype(F32)
            inv_rms = lax.rsqrt(jnp.mean(y_wide * y_wide, axis=-1, keepdims=True) + NORM_EPS)
            x_in[j * tokens:(j + 1) * tokens, :] = (y_wide * inv_rms * norm_ref[:]).astype(BF16)
        acc[:] = jnp.zeros_like(acc)

    q_all = jnp.dot(x_in[:], wq[:], preferred_element_type=F32).astype(BF16)
    k_all = jnp.dot(x_in[:], wk[:], preferred_element_type=F32).astype(BF16)
    v_all = jnp.dot(x_in[:], wv[:], preferred_element_type=F32).astype(BF16)
    causal = lax.broadcasted_iota(I32, (tokens, tokens), 0) >= lax.broadcasted_iota(I32, (tokens, tokens), 1)
    seqs = []
    for j in range(num):
        row = slice(j * tokens, (j + 1) * tokens)
        heads = []
        for h in range(wq.shape[1] // head_dim):
            part = slice(h * head_dim, (h + 1) * head_dim)
            scores = lax.dot_general(q_all[row, part], k_all[row, part], (((1,), (1,)), ((), ())), preferred_element_type=F32) * (head_dim ** -0.5)
            scores = jnp.where(causal, scores, -jnp.inf)
            weight = jnp.exp(scores - jnp.max(scores, axis=-1, keepdims=True))
            probs = (weight * (1.0 / jnp.sum(weight, axis=-1, keepdims=True))).astype(BF16)
            heads.append(jnp.dot(probs, v_all[row, part], preferred_element_type=F32).astype(BF16))
        seqs.append(jnp.concatenate(heads, axis=1))
    acc[:] += jnp.dot(jnp.concatenate(seqs, axis=0), wo[:], preferred_element_type=F32)

    @pl.when(step == last)
    def _():
        for j in range(num):
            mixed = acc[j * tokens:(j + 1) * tokens, :].astype(BF16).astype(F32)
            out[j, 0] = (ys[j][:].astype(F32) + mixed).astype(BF16)


def attend(tok, done, pair, shape, ys, norm_w, wq, wk, wv, wo):
    num = len(ys)
    tokens, d_model = ys[0].shape
    qkv = wq.shape[1]
    group = 512
    col = pl.BlockSpec((d_model, group), lambda g: (0, g))
    whole = pl.BlockSpec((tokens, d_model), lambda g: (0, 0))
    return pl.pallas_call(
        functools.partial(attn_body, num),
        out_shape=jax.ShapeDtypeStruct(shape, BF16),
        grid=(qkv // group,),
        input_output_aliases={} if done is None else {num + 6: 0},
        in_specs=[TOKEN] + [whole] * num + [pl.BlockSpec((1, d_model), lambda g: (0, 0)), col, col, col, pl.BlockSpec((group, d_model), lambda g: (g, 0))] + ([] if done is None else [TOKEN]),
        out_specs=pl.BlockSpec((num, 1, tokens, d_model), lambda g: (pair, 0, 0, 0)),
        scratch_shapes=[pltpu.VMEM((num * tokens, d_model), BF16), pltpu.VMEM((num * tokens, d_model), F32)],
        compiler_params=pltpu.CompilerParams(vmem_limit_bytes=VMEM_LIMIT),
        cost_estimate=cost(num * tokens * 4 * d_model * qkv, 4 * d_model * qkv),
        name="attend",
    )(tok, *ys, norm_w, wq, wk, wv, wo, *(() if done is None else (done,)))


def solution(mesh):
    stages = mesh.shape['pp']
    group_size = mesh.shape['ep']
    send_next = [(src_row, (src_row + 1) % stages) for src_row in range(stages)]
    tok_spec = P('pp', 'ep', None, None)
    wt_spec = P('pp', None, None, None)

    def across(x, m):
        return lax.ppermute(x, 'ep', [(i, i ^ m) for i in range(group_size)])

    def dense_path(expert_out, expert_ids, slot_ids, gate_vals, residual, norm_w, w_query, w_key, w_value, w_out):
        num_micro, seqs_dev, seq_len, d_model = residual.shape
        src_slots = expert_out.shape[2] // group_size
        returned = lax.all_to_all(expert_out, 'ep', 2, 1, tiled=True)
        block_base = lax.axis_index('ep') * src_slots
        slot_pos = jnp.where(slot_ids >= 0, slot_ids - block_base, -1)
        combined = gated_sum(returned, expert_ids, slot_pos, gate_vals, residual)
        arrived = lax.ppermute(combined, 'pp', send_next)
        flat_in = arrived.reshape(num_micro * seqs_dev, seq_len, d_model)
        result = attention_block(flat_in, norm_w[0], w_query[0], w_key[0], w_value[0], w_out[0])
        return result.reshape(num_micro, seqs_dev, seq_len, d_model)

    def device_step(expert_out, expert_ids, slot_ids, gate_vals, residual, norm_w, w_query, w_key, w_value, w_out):
        num_micro = residual.shape[0]
        me, pp = lax.axis_index('ep'), lax.axis_index('pp')
        num_exp, cap = expert_out.shape[1:3]
        d_model = expert_out.shape[3]
        src_slots = cap // group_size
        width = num_exp * src_slots
        dv = jnp.stack([me, me ^ 2, me ^ 4, me ^ 6, me * width, (me ^ 1) * width, (me ^ 2) // 2 * CHIP_STRIDE, (me ^ 4) // 2 * CHIP_STRIDE])
        idx, slot, gate = expert_ids[:, 0], slot_ids[:, 0], gate_vals[:, 0]
        table = route(me, idx, slot)
        first = sibling_slots(dv, table, 0, expert_out)
        second = sibling_slots(dv, first, 1, expert_out)
        early = across(first, 1), across(second, 1)
        everyone = lax.all_gather(table, ('pp', 'ep'))
        overflow = jnp.max(everyone[:, 8 + num_micro]) > 0

        def packed_path(everyone, table, dv, idx, slot, gate, tok, sib0, sib1, expert_out, expert_ids, slot_ids, gate_vals, residual, norm_w, w_query, w_key, w_value, w_out):
            places = stream_places(me, pp, everyone, width)
            wo = w_out[0].reshape(-1, d_model)
            sib, wide, leaf_x, leaf_y, tokens_meta, parts, arrived, outs = [sib0, sib1], [], [], [], [], {}, {}, {}

            def slots(r):
                part = sibling_slots(dv, tok, r, expert_out)
                sib.append(across(part, 1))
                return part

            def flat(weights):
                wide.extend(flat_weights(tok, weights))
                return wide[-1]

            def pack(c):
                rows = [r for r in (c, c + 1) if r < num_micro]
                to_x, to_y = pack_chunk(dv, tok, expert_out, sib, places, rows, CUTS[c], CUTS[c + 1] - CUTS[c])
                leaf_x.append(across(to_x, 2))
                leaf_y.append(across(to_y, 4))
                return to_x

            def describe(_):
                meta = token_meta(me, tok, idx, slot, gate, table)
                tokens_meta.extend([meta, across(meta, 2), across(meta, 4)])
                return meta

            def mid(r):
                chunk_ids = [c for c in (r - 1, r) if c >= 0]
                part_a, part_b = mid_sums(dv, tok, r, tokens_meta[1], tokens_meta[2], expert_out, sib, leaf_x, leaf_y, chunk_ids)
                parts[r] = across(part_a, 2), across(part_b, 4)
                return part_a

            def fin(r):
                chunk_ids = [c for c in (r - 1, r) if c >= 0]
                y = fin_sums(dv, tok, r, tokens_meta[0], expert_out, sib, leaf_x, leaf_y, chunk_ids, *parts[r], residual)
                arrived[r] = lax.ppermute(y, 'pp', send_next)
                return y

            def att(rows):
                ys = [arrived[r] for r in rows]
                outs[0] = attend(norm_w if tok is outs.get(0) else tok, outs.get(0), rows[0] // len(rows), residual.shape, ys, norm_w, *wide, wo)
                return outs[0]

            for step, what in ((pack, 0), (slots, 2), (describe, ()), (pack, 1), (slots, 3), (slots, 4), (pack, 2),
                               (flat, (w_query, w_key, w_value)), (mid, 0), (slots, 5), (pack, 3), (mid, 1), (fin, 0), (mid, 2),
                               (fin, 1), (pack, 4), (mid, 3), (pack, 5), (att, (0, 1)), (fin, 2), (mid, 4), (fin, 3), (mid, 5),
                               (fin, 4), (fin, 5), (att, (2, 3)), (att, (4, 5))):
                tok = step(what)
            return outs[0]

        args = (expert_out, expert_ids, slot_ids, gate_vals, residual, norm_w, w_query, w_key, w_value, w_out)
        return lax.cond(overflow, lambda everyone, table, dv, idx, slot, gate, tok, sib0, sib1, *a: dense_path(*a), packed_path, everyone, table, dv, idx, slot, gate, second, *early, *args)

    return jax.shard_map(device_step, mesh=mesh, in_specs=(tok_spec, tok_spec, tok_spec, tok_spec, tok_spec, P('pp', None), wt_spec, wt_spec, wt_spec, wt_spec), out_specs=tok_spec, check_vma=False)
```
